32 devices in a mesh: dp: 1 (over z), sp: 32 (over y, x, core).
Axes of the slice: x: 4, y: 4, z: 1, core: 2. Of those that a mesh axis runs over, the one named last changes fastest.
The devices are a block of a 4x4x8 slice.
Arguments:
- x: bfloat16 [4, 8192], P('dp')
- wq: bfloat16 [8192, 8192], replicated
- wk: bfloat16 [8192, 1024], replicated
- wv: bfloat16 [8192, 1024], replicated
- wo: bfloat16 [8192, 8192], P('sp')
- kc: bfloat16 [4, 32768, 8, 128], P('dp', 'sp')
- vc: bfloat16 [4, 32768, 8, 128], P('dp', 'sp')
- pos: int32 [4], P('dp')
- lens: int32 [4], P('dp')
Outputs:
- output 1: bfloat16 [4, 8192], P('dp')
- output 2: bfloat16 [4, 32768, 8, 128], P('dp', 'sp')
- output 3: bfloat16 [4, 32768, 8, 128], P('dp', 'sp')
All inputs are finite; a program needn't handle non-finite values.
Results may differ from the reference program's by a relative error of at most 0.00358209.
Values are sent between devices in bfloat16 or wider.
A program may use at most 768 MiB of HBM per device.

```python
import math
import jax
import jax.numpy as jnp
from jax import lax

B = 4
S = 32768
D = 8192
HEADS = 64
KV_HEADS = 8
HEAD = 128

G = HEADS // KV_HEADS
RCH = min(S, 2048)


def _cache(key, phase, noise):
    ka, kn = jax.random.split(key)
    nf = phase.shape[0]
    amp = jax.random.normal(ka, (B, KV_HEADS, nf, HEAD), jnp.float32) * (2.0 / nf) ** 0.5
    freq = jnp.arange(1, nf + 1).astype(jnp.float32)
    nc = S // RCH

    def piece(i):
        t = ((i % nc) * RCH + jnp.arange(RCH)).astype(jnp.float32) / S
        phi = jnp.cos(2.0 * math.pi * freq[None, :] * t[:, None] + phase[None, :])
        smooth = jnp.einsum('tf,kfd->tkd', phi, amp[i // nc])
        z = jax.random.normal(jax.random.fold_in(kn, i), (RCH, KV_HEADS, HEAD), jnp.float32)
        return (smooth + noise * z).astype(jnp.bfloat16)

    return lax.map(piece, jnp.arange(B * nc)).reshape(B, S, KV_HEADS, HEAD)


def setup_inputs(seed: int = 0, part: int = 0) -> dict:
    ks = jax.random.split(jax.random.PRNGKey(seed), 12)
    pk = [jax.random.fold_in(k, part) for k in ks[5:]]
    u = jax.random.normal(ks[0], (D, KV_HEADS, 1, HEAD), jnp.float32)
    wq = (u + jax.random.normal(ks[1], (D, KV_HEADS, G, HEAD), jnp.float32)) * (2.0 * D) ** -0.5
    gamma = math.log(0.1 * S) * (2.0 / HEAD) ** 0.5
    wk = (gamma * u[:, :, 0] + 0.5 * jax.random.normal(ks[2], (D, KV_HEADS, HEAD), jnp.float32)) * D ** -0.5
    wv = jax.random.normal(ks[3], (D, KV_HEADS * HEAD), jnp.float32) * D ** -0.5
    wo = jax.random.normal(ks[4], (HEADS * HEAD, D), jnp.float32) * (HEADS * HEAD) ** -0.5
    x = jax.random.normal(pk[0], (B, D), jnp.float32)
    lens = jax.random.randint(pk[1], (B,), S // 32, S + 1, jnp.int32)
    kc = _cache(pk[2], jax.random.uniform(pk[3], (4,), jnp.float32, 0.0, 2.0 * math.pi), 0.6)
    vc = _cache(pk[4], jax.random.uniform(pk[5], (4,), jnp.float32, 0.0, 2.0 * math.pi), 0.5)
    return {
        'x': x.astype(jnp.bfloat16),
        'wq': wq.reshape(D, HEADS * HEAD).astype(jnp.bfloat16),
        'wk': wk.reshape(D, KV_HEADS * HEAD).astype(jnp.bfloat16),
        'wv': wv.astype(jnp.bfloat16),
        'wo': wo.astype(jnp.bfloat16),
        'kc': kc,
        'vc': vc,
        'pos': lens - 1,
        'lens': lens,
    }


def reference(x, wq, wk, wv, wo, kc, vc, pos, lens):
    q = jnp.dot(x, wq, preferred_element_type=jnp.float32).astype(jnp.bfloat16).reshape(B, KV_HEADS, G, HEAD)
    k = jnp.dot(x, wk, preferred_element_type=jnp.float32).astype(jnp.bfloat16).reshape(B, KV_HEADS, HEAD)
    v = jnp.dot(x, wv, preferred_element_type=jnp.float32).astype(jnp.bfloat16).reshape(B, KV_HEADS, HEAD)
    bi = jnp.arange(B)
    kn = kc.at[bi, pos].set(k)
    vn = vc.at[bi, pos].set(v)
    qf = q.astype(jnp.float32)

    def block(c):
        kb = lax.dynamic_slice_in_dim(kn, c * RCH, RCH, axis=1).astype(jnp.float32)
        vb = lax.dynamic_slice_in_dim(vn, c * RCH, RCH, axis=1).astype(jnp.float32)
        s = jnp.einsum('bkgd,bskd->bkgs', qf, kb) * HEAD ** -0.5
        valid = (c * RCH + jnp.arange(RCH))[None, :] < lens[:, None]
        s = jnp.where(valid[:, None, None, :], s, -jnp.inf)
        m = s.max(-1)
        p = jnp.exp(s - jnp.where(jnp.isfinite(m), m, 0.0)[..., None])
        return m, p.sum(-1), jnp.einsum('bkgs,bskd->bkgd', p, vb)

    m, l, o = lax.map(block, jnp.arange(S // RCH))
    a = jnp.exp(m - m.max(0))
    out = (a[..., None] * o).sum(0) / (a * l).sum(0)[..., None]
    out = out.astype(jnp.bfloat16).reshape(B, HEADS * HEAD)
    y = jnp.dot(out, wo, preferred_element_type=jnp.float32).astype(jnp.bfloat16)
    return (y, kn, vn)
```

```python
import functools
import jax
import jax.numpy as jnp
from jax import lax
from jax.experimental import pallas as pl
from jax.experimental.pallas import tpu as pltpu
from jax.sharding import PartitionSpec as P

MESH = pl.DeviceIdType.MESH
F32 = jnp.float32
BF16 = jnp.bfloat16
NQ = 4
R = 16


def peer(n, k):
    return lax.rem(lax.axis_index('sp') + k, n)


def barrier(n):
    sem = pltpu.get_barrier_semaphore()

    def one(k, c):
        pl.semaphore_signal(sem, 1, device_id={'sp': peer(n, k)}, device_id_type=MESH)
        return c
    lax.fori_loop(1, n, one, 0)
    return sem


def far_first(n):
    return sorted(range(1, n), key=lambda k: (-min(k, n - k), k))


def all_of(refs, sem):
    pltpu.make_async_copy(refs, refs, sem).wait()


def project(n, x, wq, wk, wv, kc, vc, qall, kvn, kv, vv,
            wqb, wkvb, qs, kvs, part, theirs, wsem, csem, ps, pr, qss, qrs, kss, krs):
    me = lax.axis_index('sp')
    d = x.shape[1]
    nb = x.shape[0]
    cols = wqb.shape[1]
    half = wkvb.shape[0]
    r = lax.rem(me, 2)
    t = lax.div(me, 2)
    heads = wk.shape[1] // 128
    bar = barrier(n)
    row0 = pl.multiple_of(r * half, half)

    @pl.when(t < heads)
    def _():
        pltpu.make_async_copy(wk.at[pl.ds(row0, half), pl.ds(pl.multiple_of(t * 128, 128), 128)], wkvb, wsem.at[NQ]).start()

    @pl.when(t >= heads)
    def _():
        pltpu.make_async_copy(wv.at[pl.ds(row0, half), pl.ds(pl.multiple_of((t - heads) * 128, 128), 128)], wkvb, wsem.at[NQ]).start()
    step = d // NQ
    wcp = [pltpu.make_async_copy(wq.at[pl.ds(i * step, step), pl.ds(pl.multiple_of(me * cols, cols), cols)],
                                 wqb.at[pl.ds(i * step, step)], wsem.at[i]) for i in range(NQ)]
    for c in wcp:
        c.start()
    ccp = [pltpu.make_async_copy(kc, kv, csem.at[0]), pltpu.make_async_copy(vc, vv, csem.at[1])]
    for c in ccp:
        c.start()
    pltpu.make_async_copy(wk.at[pl.ds(0, half), pl.ds(0, 128)], wkvb, wsem.at[NQ]).wait()
    kvp = jnp.dot(x[:, pl.ds(row0, half)], wkvb[...], preferred_element_type=F32)
    part[...] = jnp.concatenate([kvp, kvp], axis=0)
    pl.semaphore_wait(bar, n - 1)
    swap = pltpu.make_async_remote_copy(part, theirs, ps, pr, device_id={'sp': me + 1 - 2 * r}, device_id_type=MESH)
    q = jnp.zeros((nb, cols), F32)
    for i in range(NQ):
        wcp[i].wait()
        q = q + jnp.dot(x[:, i * step:(i + 1) * step], wqb[i * step:(i + 1) * step], preferred_element_type=F32)
        if i == 0:
            swap.start()
    qs[...] = jnp.concatenate([q[:, :128], q[:, 128:]], axis=0).astype(BF16)
    qall[me] = qs[...]
    swap.wait()
    kvs[...] = (part[...] + theirs[...]).astype(BF16)
    kvn[t] = kvs[...]

    def sendq(k, c):
        pltpu.make_async_remote_copy(qs, qall.at[me], qss, qrs, device_id={'sp': peer(n, k)}, device_id_type=MESH).start()
        return c
    lax.fori_loop(1, n, sendq, 0)

    def sendkv(k, c):
        pltpu.make_async_remote_copy(kvs, kvn.at[t], kss, krs, device_id={'sp': peer(n, 2 * k)}, device_id_type=MESH).start()
        return c
    lax.fori_loop(1, n // 2, sendkv, 0)
    all_of(qall.at[pl.ds(0, n - 1)], qss)
    all_of(kvn.at[pl.ds(0, n // 2 - 1)], kss)
    all_of(qall.at[pl.ds(0, n - 1)], qrs)
    all_of(kvn.at[pl.ds(0, n // 2 - 1)], krs)
    for c in ccp:
        c.wait()


def attend(n, pos, qall, kvn, kv, vv, ko, vo, om, qb, s_ref, ob, gb, rw, wsem, rsem):
    me = lax.axis_index('sp')
    nb, rows, dh = kv.shape
    hk = 8
    sl = rows // hk
    nh = 2 * n
    start = me * sl
    cp = []
    for b in range(nb):
        cp.append((pltpu.make_async_copy(kv.at[b], ko.at[b], wsem.at[0, b]),
                   pltpu.make_async_copy(vv.at[b], vo.at[b], wsem.at[1, b])))
    for c in cp:
        c[0].start()
        c[1].start()
    m_ = nb * nh
    i0 = lax.broadcasted_iota(jnp.int32, (m_, m_), 0)
    i1 = lax.broadcasted_iota(jnp.int32, (m_, m_), 1)
    want = (lax.rem(i0, nh) // 2) * (2 * nb) + lax.rem(i0, 2) * nb + i0 // nh
    perm = (i1 == want).astype(F32).astype(BF16)
    qb[...] = jnp.dot(perm, qall[...].reshape(m_, dh), preferred_element_type=F32).astype(BF16)
    nt = kvn.shape[0]
    j0 = lax.broadcasted_iota(jnp.int32, (nt * nb, nt * 2 * nb), 0)
    j1 = lax.broadcasted_iota(jnp.int32, (nt * nb, nt * 2 * nb), 1)
    want2 = ((j0 // (nb * hk)) * hk + lax.rem(j0, hk)) * 2 * nb + lax.rem(j0 // hk, nb)
    perm2 = (j1 == want2).astype(F32).astype(BF16)
    rw[...] = jnp.dot(perm2, kvn[...].reshape(nt * 2 * nb, dh), preferred_element_type=F32).astype(BF16).reshape(2 * nb, hk, dh)
    ch = 1024
    row = lax.broadcasted_iota(jnp.int32, (nh, ch), 0) // hk
    lane = lax.broadcasted_iota(jnp.int32, (nh, ch), 1)
    diag = row == lax.rem(lane, hk)
    glane = lax.broadcasted_iota(jnp.int32, (nh, dh), 1)
    ghalf = lax.rem(lax.broadcasted_iota(jnp.int32, (nh, dh), 0), 2)
    g = jnp.zeros((nh, dh), F32)
    c = dh ** -0.5
    for b in range(nb):
        lim = (pos[b] - start) * hk
        q = qb[b * nh:(b + 1) * nh]
        mx = jnp.full((nh, 1), -jnp.inf, F32)
        for i in range(rows // ch):
            s = lax.dot_general(q, kv[b, i * ch:(i + 1) * ch], (((1,), (1,)), ((), ())), preferred_element_type=F32) * c
            s = jnp.where(diag & (lane < lim - i * ch), s, -jnp.inf)
            mx = jnp.maximum(mx, s.max(1, keepdims=True))
            s_ref[:, i * ch:(i + 1) * ch] = s
        safe = jnp.where(mx == -jnp.inf, 0.0, mx)
        l = jnp.zeros((nh, 1), F32)
        o = jnp.zeros((nh, dh), F32)
        for i in range(rows // ch):
            p = jnp.exp(s_ref[:, i * ch:(i + 1) * ch] - safe)
            l = l + p.sum(1, keepdims=True)
            o = o + jnp.dot(p.astype(BF16), vv[b, i * ch:(i + 1) * ch], preferred_element_type=F32)
        ob[...] = o
        for h in range(2):
            om[pl.ds(h * nb + b, n, stride=R), :] = ob[pl.ds(h, n, stride=2), :]
        g = g + jnp.where(glane == ghalf * nb + b, mx, 0.0) + jnp.where(glane == 2 * nb + ghalf * nb + b, l, 0.0)
    gb[...] = g
    stat = gb[pl.ds(0, n, stride=2), :]
    stat2 = gb[pl.ds(1, n, stride=2), :]
    gl = lax.rem(lax.broadcasted_iota(jnp.int32, (n, dh), 1), 2 * nb)
    om[pl.ds(2 * nb, n, stride=R), :] = jnp.where(gl < nb, stat, stat2)
    for b in range(nb):
        cp[b][0].wait()
        cp[b][1].wait()
    for b in range(nb):
        at = pos[b] - start

        @pl.when((at >= 0) & (at < sl))
        def _():
            k1 = pltpu.make_async_copy(rw.at[b], ko.at[b, pl.ds(at * hk, hk)], rsem.at[0])
            k2 = pltpu.make_async_copy(rw.at[nb + b], vo.at[b, pl.ds(at * hk, hk)], rsem.at[1])
            k1.start()
            k2.start()
            k1.wait()
            k2.wait()


def finish(n, qall, kvn, om, wo, yo, wob, orx, ys, yrx, yb, wsem, os_, or_, ys_, yr_, gs_, gr_):
    me = lax.axis_index('sp')
    dh = qall.shape[2]
    hk = kvn.shape[0] // 2
    nb = 4
    cols = wo.shape[1] // n
    bar = barrier(n)
    wcp = pltpu.make_async_copy(wo, wob, wsem)
    wcp.start()
    pl.semaphore_wait(bar, n - 1)

    def slot(i, r):
        return pl.ds(pl.multiple_of(i * r, r), r)

    def sendo(k, c):
        to = peer(n, k)
        pltpu.make_async_remote_copy(om.at[slot(to, R)], orx.at[slot(me, R)], os_, or_,
                                     device_id={'sp': to}, device_id_type=MESH).start()
        return c
    lax.fori_loop(1, n, sendo, 0)
    orx[slot(me, R), :] = om[slot(me, R), :]
    kh = lax.div(me * hk, n)
    knew = kvn[kh].astype(F32)
    vnew = kvn[hk + kh].astype(F32)
    snew = (qall[me].astype(F32) * knew).sum(1, keepdims=True) * dh ** -0.5
    all_of(om.at[pl.ds(0, (n - 1) * R)], os_)
    all_of(orx.at[pl.ds(0, (n - 1) * R)], or_)
    st = orx[pl.ds(2 * nb, n, stride=R), :].T
    m = st[0:2 * nb]
    l = st[2 * nb:4 * nb]
    top = jnp.maximum(m.max(1, keepdims=True), snew)
    a = jnp.exp(m - top)
    anew = jnp.exp(snew - top)
    den = (a * l).sum(1, keepdims=True) + anew
    num = anew * vnew
    for i in range(n):
        num = num + a[:, i:i + 1] * orx[i * R:i * R + 2 * nb, :]
    o = (num / den)
    o = jnp.concatenate([o[:nb], o[nb:]], axis=1).astype(BF16)
    wcp.wait()
    order = far_first(n) + [0]
    for g in range(0, n, 8):
        for k in order[g:g + 8]:
            to = peer(n, k)
            w = wob[:, pl.ds(pl.multiple_of(to * cols, cols), cols)]
            part = jnp.dot(o, w, preferred_element_type=F32)
            part = jnp.concatenate([part[:, :128], part[:, 128:]], axis=0)
            if k:
                ys[to] = part
            else:
                yrx[me] = part
        for k in order[g:g + 8]:
            if k:
                to = peer(n, k)
                pltpu.make_async_remote_copy(ys.at[to], yrx.at[me], ys_, yr_, device_id={'sp': to}, device_id_type=MESH).start()
    all_of(ys.at[pl.ds(0, n - 1)], ys_)
    all_of(yrx.at[pl.ds(0, n - 1)], yr_)
    yb[...] = yrx[...].sum(0).astype(BF16)
    yo[me] = yb[...]

    def sendy(k, c):
        to = peer(n, k)
        pltpu.make_async_remote_copy(yb, yo.at[me], gs_, gr_, device_id={'sp': to}, device_id_type=MESH).start()
        return c
    lax.fori_loop(1, n, sendy, 0)
    all_of(yo.at[pl.ds(0, n - 1)], gs_)
    all_of(yo.at[pl.ds(0, n - 1)], gr_)


def solution(mesh):
    n = mesh.shape['sp']
    vm = pl.BlockSpec(memory_space=pltpu.VMEM)
    hbm = pl.BlockSpec(memory_space=pltpu.HBM)
    sm = pl.BlockSpec(memory_space=pltpu.SMEM)
    dma = pltpu.SemaphoreType.DMA

    def params(i, mib):
        return pltpu.CompilerParams(collective_id=i, has_side_effects=i is not None, vmem_limit_bytes=mib * 2**20)

    def local(x, wq, wk, wv, wo, kc, vc, pos, lens):
        nb, d = x.shape
        _, sl, hk, dh = kc.shape
        cols = wq.shape[1] // n
        nt = 2 * hk
        half = d * nt // n
        kc = kc.reshape(nb, sl * hk, dh)
        vc = vc.reshape(nb, sl * hk, dh)
        shape = kc.shape
        wq, wk, wv, wo, kc, vc = (pltpu.with_memory_space_constraint(a, pltpu.HBM) for a in (wq, wk, wv, wo, kc, vc))
        qall, kvn, kv, vv = pl.pallas_call(
            functools.partial(project, n),
            out_shape=[pltpu.VMEM((n, 2 * nb, dh), BF16), pltpu.VMEM((nt, 2 * nb, dh), BF16),
                       pltpu.VMEM(shape, BF16), pltpu.VMEM(shape, BF16)],
            in_specs=[vm, hbm, hbm, hbm, hbm, hbm], out_specs=[vm] * 4,
            scratch_shapes=[pltpu.VMEM((d, cols), BF16), pltpu.VMEM((half, dh), BF16),
                            pltpu.VMEM((2 * nb, dh), BF16), pltpu.VMEM((2 * nb, dh), BF16),
                            pltpu.VMEM((2 * nb, dh), F32), pltpu.VMEM((2 * nb, dh), F32),
                            dma((NQ + 1,)), dma((2,))] + [dma] * 6,
            compiler_params=params(0, 16), name='project')(x, wq, wk, wv, kc, vc)
        ko, vo, om = pl.pallas_call(
            functools.partial(attend, n),
            out_shape=[jax.ShapeDtypeStruct(shape, BF16), jax.ShapeDtypeStruct(shape, BF16), pltpu.VMEM((n * R, dh), F32)],
            in_specs=[sm, vm, vm, vm, vm], out_specs=[hbm, hbm, vm],
            scratch_shapes=[pltpu.VMEM((n * 2 * nb, dh), BF16), pltpu.VMEM((2 * n, sl * hk), F32),
                            pltpu.VMEM((2 * n, dh), F32), pltpu.VMEM((2 * n, dh), F32), pltpu.VMEM((2 * nb, hk, dh), BF16),
                            dma((2, nb)), dma((2,))],
            compiler_params=params(None, 16), name='attend')(pos, qall, kvn, kv, vv)
        y = pl.pallas_call(
            functools.partial(finish, n),
            out_shape=jax.ShapeDtypeStruct((n, 2 * nb, dh), BF16),
            in_specs=[vm, vm, vm, hbm], out_specs=vm,
            scratch_shapes=[pltpu.VMEM(wo.shape, BF16), pltpu.VMEM((n * R, dh), F32), pltpu.VMEM((n, 2 * nb, dh), F32),
                            pltpu.VMEM((n, 2 * nb, dh), F32), pltpu.VMEM((2 * nb, dh), BF16)] + [dma] * 7,
            compiler_params=params(1, 16), name='finish')(qall, kvn, om, wo)
        y = y.reshape(n, 2, nb, dh).transpose(2, 0, 1, 3).reshape(nb, -1)
        return y, ko.reshape(nb, sl, hk, dh), vo.reshape(nb, sl, hk, dh)

    cache = P('dp', 'sp', None, None)
    return jax.shard_map(
        local, mesh=mesh,
        in_specs=(P('dp', None), P(None, None), P(None, None), P(None, None), P('sp', None),
                  cache, cache, P('dp'), P('dp')),
        out_specs=(P('dp', None), cache, cache),
        check_vma=False)
```

```python
import functools
import math
import jax
import jax.numpy as jnp
from jax import lax
from jax.experimental import pallas as pl
from jax.experimental.pallas import tpu as pltpu
from jax.sharding import PartitionSpec as P

MESH = pl.DeviceIdType.MESH
F32 = jnp.float32
BF16 = jnp.bfloat16
NQ = 8
CT = 1024
CH = 512
R = 9


def peer(n, k):
    return lax.rem(lax.axis_index('sp') + k, n)


def far_first(n, ks):
    side = max(1, math.isqrt(n // 2))

    def hops(k):
        a, b = (k // 2) % side, (k // 2) // side
        return min(a, side - a) + min(b, side - b)
    return sorted(ks, key=lambda k: (-hops(k), k))


def barrier(n):
    sem = pltpu.get_barrier_semaphore()
    for k in far_first(n, range(1, n)):
        pl.semaphore_signal(sem, 1, device_id={'sp': peer(n, k)}, device_id_type=MESH)
    return sem


def all_of(refs, sem):
    pltpu.make_async_copy(refs, refs, sem).wait()


class Softmax:
    def __init__(self, q2, kt, vb, lim, s_ref, hk):
        nh, dh = q2.shape[0] // 2, q2.shape[1] // 2
        self.nh, self.dh, self.kt, self.vb, self.lim, self.s = nh, dh, kt, vb, lim, s_ref
        self.c2 = dh ** -0.5 * math.log2(math.e)
        self.q2 = q2
        row = lax.broadcasted_iota(jnp.int32, (nh, 128), 0) // hk
        self.lane = lax.broadcasted_iota(jnp.int32, (nh, 128), 1)
        self.bias = jnp.where(row == lax.rem(self.lane, hk), 0.0, -jnp.inf)
        self.mx = jnp.full((nh, 128), -jnp.inf, F32)
        self.l = jnp.zeros((nh, 128), F32)
        self.o = jnp.zeros((2 * nh, 2 * dh), F32)

    def scores(self, i):
        nh, half = self.nh, CH // 2
        k2 = jnp.concatenate([self.kt[:, i:i + half], self.kt[:, i + half:i + CH]], axis=0)
        s = jnp.dot(self.q2[...], k2, preferred_element_type=F32)
        for u in range(2):
            for e in range(0, half, 128):
                se = jnp.where(self.lane < self.lim - (i + u * half + e), s[u * nh:(u + 1) * nh, e:e + 128] + self.bias, -jnp.inf)
                self.mx = jnp.maximum(self.mx, se)
                self.s[u * nh:(u + 1) * nh, i // 2 + e:i // 2 + e + 128] = se

    def maximum(self):
        self.m = self.mx.max(1, keepdims=True) * self.c2
        self.safe = jnp.where(self.m == -jnp.inf, 0.0, self.m)

    def values(self, i):
        nh, half = self.nh, CH // 2
        ps = []
        for u in range(2):
            row = []
            for e in range(0, half, 128):
                p = jnp.exp2(self.s[u * nh:(u + 1) * nh, i // 2 + e:i // 2 + e + 128] * self.c2 - self.safe)
                self.l = self.l + p
                row.append(p.astype(BF16))
            ps.append(jnp.concatenate(row, axis=1))
        v2 = jnp.concatenate([self.vb[i:i + half], self.vb[i + half:i + CH]], axis=1)
        self.o = self.o + jnp.dot(jnp.concatenate(ps, axis=0), v2, preferred_element_type=F32)

    def result(self):
        nh, dh = self.nh, self.dh
        return self.m, self.l.sum(1, keepdims=True), self.o[:nh, :dh] + self.o[nh:, dh:]


def put(n, nb, b, m, l, o, om, ob):
    nh, dh = o.shape
    ob[...] = o
    for h in range(2):
        om[:, h * nb + b, :] = ob[pl.ds(h, n, stride=2), :]
    glane = lax.broadcasted_iota(jnp.int32, (nh, dh), 1)
    at = lax.rem(lax.broadcasted_iota(jnp.int32, (nh, dh), 0), 2) * nb + b
    return jnp.where(glane == at, m, 0.0) + jnp.where(glane == 2 * nb + at, l, 0.0)


def stats_row(n, g, gb):
    gb[...] = g
    return gb[pl.ds(0, n, stride=2), :] + gb[pl.ds(1, n, stride=2), :]


def decode(n, posh, x, wq, wk, wv, wo, kc, vc, yo, rw, kv, vv,
           qall, kvn, xb, wqb, wkvb, qs, kvs, part, theirs, perm_ref, q2, kt, s_ref, ob, gb, om, wob, orx, ys, yrx, yb,
           pos, psem, xsem, wsem, csem, osem, ps, pr, qss, qrs, kss, krs, os_, or_, ys_, yr_, gs_, gr_):
    me = lax.axis_index('sp')
    nb, d = x.shape
    cols = wqb.shape[1]
    half = wkvb.shape[0]
    r = lax.rem(me, 2)
    t = lax.div(me, 2)
    heads = wk.shape[1] // 128
    row0 = pl.multiple_of(r * half, half)
    xcp = pltpu.make_async_copy(x, xb, xsem)
    xcp.start()
    pcp = pltpu.make_async_copy(posh, pos, psem)
    pcp.start()

    @pl.when(t < heads)
    def _():
        pltpu.make_async_copy(wk.at[pl.ds(row0, half), pl.ds(pl.multiple_of(t * 128, 128), 128)], wkvb, wsem.at[NQ]).start()

    @pl.when(t >= heads)
    def _():
        pltpu.make_async_copy(wv.at[pl.ds(row0, half), pl.ds(pl.multiple_of((t - heads) * 128, 128), 128)], wkvb, wsem.at[NQ]).start()
    step = d // NQ
    wcp = [pltpu.make_async_copy(wq.at[pl.ds(i * step, step), pl.ds(pl.multiple_of(me * cols, cols), cols)],
                                 wqb.at[pl.ds(i * step, step)], wsem.at[i]) for i in range(NQ)]
    for c in wcp:
        c.start()
    bar = barrier(n)
    ccp = [pltpu.make_async_copy(f.at[b], t_.at[b], csem.at[e, b]) for e, (f, t_) in enumerate(((kc, kv), (vc, vv)))
           for b in range(nb)]
    xcp.wait()
    pcp.wait()
    pltpu.make_async_copy(wk.at[pl.ds(0, half), pl.ds(0, 128)], wkvb, wsem.at[NQ]).wait()
    kvp = jnp.dot(xb[:, pl.ds(row0, half)], wkvb[...], preferred_element_type=F32)
    part[...] = jnp.concatenate([kvp, kvp], axis=0)
    swap = pltpu.make_async_remote_copy(part, theirs, ps, pr, device_id={'sp': me + 1 - 2 * r}, device_id_type=MESH)
    q = jnp.zeros((nb, cols), F32)
    for i in range(NQ):
        wcp[i].wait()
        if i == NQ - 3:
            for c in ccp[:nb]:
                c.start()
        q = q + jnp.dot(xb[:, i * step:(i + 1) * step], wqb[i * step:(i + 1) * step], preferred_element_type=F32)
    qs[...] = jnp.concatenate([q[:, :128], q[:, 128:]], axis=0).astype(BF16)
    qall[me] = qs[...]
    pl.semaphore_wait(bar, n - 1)
    swap.start()

    for k in far_first(n, range(1, n)):
        pltpu.make_async_remote_copy(qs, qall.at[me], qss, qrs, device_id={'sp': peer(n, k)}, device_id_type=MESH).start()
    swap.wait()
    kvs[...] = (part[...] + theirs[...]).astype(BF16)
    kvn[t] = kvs[...]

    for k in far_first(n, range(2, n, 2)):
        pltpu.make_async_remote_copy(kvs, kvn.at[t], kss, krs, device_id={'sp': peer(n, k)}, device_id_type=MESH).start()
    wcp_o = pltpu.make_async_copy(wo, wob, osem)
    _, rows, dh = kv.shape
    hk = rw.shape[1]
    sl = rows // hk
    nh = 2 * n
    start = me * sl
    m_ = nb * nh
    i0 = lax.broadcasted_iota(jnp.int32, (m_, m_), 0)
    i1 = lax.broadcasted_iota(jnp.int32, (m_, m_), 1)
    want = (lax.rem(i0, nh) // 2) * (2 * nb) + lax.rem(i0, 2) * nb + i0 // nh
    perm_ref[...] = (i1 == want).astype(F32).astype(BF16)
    for b in range(nb):
        ccp[b].wait()
        ccp[nb + b].start()
        for i in range(0, kv.shape[1], CT):
            kt[b, :, i:i + CT] = kv[b, i:i + CT].T
    all_of(qall.at[pl.ds(0, n - 1)], qrs)
    wcp_o.start()
    qb = jnp.dot(perm_ref[...], qall[...].reshape(m_, dh), preferred_element_type=F32).astype(BF16)
    for b in range(nb):
        for u in range(2):
            q2[b, u * nh:(u + 1) * nh, u * dh:(u + 1) * dh] = qb[b * nh:(b + 1) * nh]
            q2[b, u * nh:(u + 1) * nh, (1 - u) * dh:(2 - u) * dh] = jnp.zeros((nh, dh), BF16)
    g = jnp.zeros((nh, dh), F32)
    at = [Softmax(q2.at[b], kt.at[b], vv.at[b], (pos[b] - start) * hk, s_ref.at[b % 2], hk) for b in range(nb)]
    for b in range(nb + 1):
        if b:
            ccp[nb + b - 1].wait()
        for i in range(0, rows, CH):
            if b < nb:
                at[b].scores(i)
            if b:
                at[b - 1].values(i)
        if b < nb:
            at[b].maximum()
        if b:
            g = g + put(n, nb, b - 1, *at[b - 1].result(), om, ob)
    om[:, 2 * nb, :] = stats_row(n, g, gb)
    cols = wo.shape[1] // n
    for k in far_first(n, range(1, n)):
        to = peer(n, k)
        pltpu.make_async_remote_copy(om.at[to], orx.at[me], os_, or_,
                                     device_id={'sp': to}, device_id_type=MESH).start()
    orx[me] = om[me]
    all_of(qall.at[pl.ds(0, n - 1)], qss)
    all_of(kvn.at[pl.ds(0, n // 2 - 1)], kss)
    all_of(kvn.at[pl.ds(0, n // 2 - 1)], krs)
    nt = kvn.shape[0]
    j0 = lax.broadcasted_iota(jnp.int32, (nt * nb, nt * 2 * nb), 0)
    j1 = lax.broadcasted_iota(jnp.int32, (nt * nb, nt * 2 * nb), 1)
    want2 = ((j0 // (nb * hk)) * hk + lax.rem(j0, hk)) * 2 * nb + lax.rem(j0 // hk, nb)
    perm2 = (j1 == want2).astype(F32).astype(BF16)
    rw[...] = jnp.dot(perm2, kvn[...].reshape(nt * 2 * nb, dh), preferred_element_type=F32).astype(BF16).reshape(2 * nb, hk, dh)
    kh = lax.div(me * hk, n)
    knew = kvn[kh].astype(F32)
    vnew = kvn[hk + kh].astype(F32)
    snew = (qall[me].astype(F32) * knew).sum(1, keepdims=True) * (dh ** -0.5 * math.log2(math.e))
    all_of(om.at[pl.ds(0, n - 1)], os_)
    all_of(orx.at[pl.ds(0, n - 1)], or_)
    st = orx[:, 2 * nb, :].T
    m = st[0:2 * nb]
    l = st[2 * nb:4 * nb]
    top = jnp.maximum(m.max(1, keepdims=True), snew)
    a = jnp.exp2(m - top)
    anew = jnp.exp2(snew - top)
    den = (a * l).sum(1, keepdims=True) + anew
    num = anew * vnew
    for i in range(n):
        num = num + a[:, i:i + 1] * orx[i, 0:2 * nb, :]
    o = (num / den)
    o = jnp.concatenate([o[:nb], o[nb:]], axis=1).astype(BF16)
    wcp_o.wait()
    order = far_first(n, range(n))
    for g in range(0, n, 8):
        for k in order[g:g + 8]:
            to = peer(n, k)
            w = wob[:, pl.ds(pl.multiple_of(to * cols, cols), cols)]
            part = jnp.dot(o, w, preferred_element_type=F32)
            part = jnp.concatenate([part[:, :128], part[:, 128:]], axis=0)
            if k:
                ys[to] = part
            else:
                yrx[me] = part
        for k in order[g:g + 8]:
            if k:
                to = peer(n, k)
                pltpu.make_async_remote_copy(ys.at[to], yrx.at[me], ys_, yr_, device_id={'sp': to}, device_id_type=MESH).start()
    all_of(ys.at[pl.ds(0, n - 1)], ys_)
    all_of(yrx.at[pl.ds(0, n - 1)], yr_)
    yb[...] = yrx[...].sum(0).astype(BF16)
    yo[me] = yb[...]

    for k in far_first(n, range(1, n)):
        pltpu.make_async_remote_copy(yb, yo.at[me], gs_, gr_, device_id={'sp': peer(n, k)}, device_id_type=MESH).start()
    all_of(yo.at[pl.ds(0, n - 1)], gs_)
    all_of(yo.at[pl.ds(0, n - 1)], gr_)


def store(n, pos, rw, y, kv, vv, ko, vo, yo, k2, v2, sem, ysem):
    nb, rows, _ = kv.shape
    hk = rw.shape[1]
    sl = rows // hk
    start = lax.axis_index('sp') * sl

    def bulk(b):
        return (pltpu.make_async_copy(k2.at[b], ko.at[b], sem.at[0, b]), pltpu.make_async_copy(v2.at[b], vo.at[b], sem.at[1, b]))

    def begin(b, own):
        at = pos[b] - start
        here = (at >= 0) & (at < sl)

        @pl.when(here if own else jnp.logical_not(here))
        def _():
            for a in bulk(b):
                a.start()
    for b in range(nb):
        at = pos[b] - start

        @pl.when((at >= 0) & (at < sl))
        def _():
            here = pl.ds(pl.multiple_of(at * hk, hk), hk)
            k2[b, here] = rw[b]
            v2[b, here] = rw[nb + b]
    for own in (False, True):
        for b in range(nb):
            begin(b, own)
    ycp = pltpu.make_async_copy(y, yo, ysem)
    ycp.start()
    ycp.wait()
    for b in range(nb):
        for a in bulk(b):
            a.wait()


def solution(mesh):
    n = mesh.shape['sp']
    vm = pl.BlockSpec(memory_space=pltpu.VMEM)
    hbm = pl.BlockSpec(memory_space=pltpu.HBM)
    sm = pl.BlockSpec(memory_space=pltpu.SMEM)
    dma = pltpu.SemaphoreType.DMA

    def params(i, mib):
        return pltpu.CompilerParams(collective_id=i, has_side_effects=i is not None, vmem_limit_bytes=mib * 2**20)

    def local(x, wq, wk, wv, wo, kc, vc, pos, lens):
        nb, d = x.shape
        _, sl, hk, dh = kc.shape
        cols = wq.shape[1] // n
        nt = 2 * hk
        half = d * nt // n
        kc = kc.reshape(nb, sl * hk, dh)
        vc = vc.reshape(nb, sl * hk, dh)
        shape = kc.shape
        x, wq, wk, wv, wo, kc, vc = (pltpu.with_memory_space_constraint(a, pltpu.HBM) for a in (x, wq, wk, wv, wo, kc, vc))
        small = (2 * nb, dh)
        y, rw, kv, vv = pl.pallas_call(
            functools.partial(decode, n),
            out_shape=[pltpu.VMEM((n,) + small, BF16), pltpu.VMEM((2 * nb, hk, dh), BF16), pltpu.VMEM(shape, BF16), pltpu.VMEM(shape, BF16)],
            in_specs=[hbm] * 8, out_specs=[vm] * 4,
            scratch_shapes=[pltpu.VMEM((n,) + small, BF16), pltpu.VMEM((nt,) + small, BF16),
                            pltpu.VMEM((nb, d), BF16), pltpu.VMEM((d, cols), BF16), pltpu.VMEM((half, dh), BF16),
                            pltpu.VMEM(small, BF16), pltpu.VMEM(small, BF16), pltpu.VMEM(small, F32), pltpu.VMEM(small, F32),
                            pltpu.VMEM((n * 2 * nb, n * 2 * nb), BF16), pltpu.VMEM((nb, 4 * n, 2 * dh), BF16), pltpu.VMEM((nb, dh, sl * hk), BF16), pltpu.VMEM((2, 4 * n, sl * hk // 2), F32),
                            pltpu.VMEM((2 * n, dh), F32), pltpu.VMEM((2 * n, dh), F32), pltpu.VMEM((n, R, dh), F32),
                            pltpu.VMEM(wo.shape, BF16), pltpu.VMEM((n, R, dh), F32), pltpu.VMEM((n,) + small, F32),
                            pltpu.VMEM((n,) + small, F32), pltpu.VMEM(small, BF16),
                            pltpu.SMEM((nb,), jnp.int32), dma, dma, dma((NQ + 1,)), dma((2, nb)), dma] + [dma] * 12,
            compiler_params=params(0, 36), name='decode')(pltpu.with_memory_space_constraint(pos, pltpu.HBM), x, wq, wk, wv, wo, kc, vc)
        ko, vo, y, _, _ = pl.pallas_call(
            functools.partial(store, n),
            out_shape=[jax.ShapeDtypeStruct(shape, BF16), jax.ShapeDtypeStruct(shape, BF16), jax.ShapeDtypeStruct(y.shape, BF16),
                       pltpu.VMEM(shape, BF16), pltpu.VMEM(shape, BF16)],
            in_specs=[sm, vm, vm, vm, vm], out_specs=[hbm, hbm, hbm, vm, vm],
            input_output_aliases={3: 3, 4: 4},
            scratch_shapes=[dma((2, nb)), dma],
            compiler_params=params(None, 4), name='store')(pos, rw, y, kv, vv)
        y = y.reshape(n, 2, nb, dh).transpose(2, 0, 1, 3).reshape(nb, -1)
        return y, ko.reshape(nb, sl, hk, dh), vo.reshape(nb, sl, hk, dh)

    cache = P('dp', 'sp', None, None)
    return jax.shard_map(
        local, mesh=mesh,
        in_specs=(P('dp', None), P(None, None), P(None, None), P(None, None), P('sp', None),
                  cache, cache, P('dp'), P('dp')),
        out_specs=(P('dp', None), cache, cache),
        check_vma=False)
```

```python
import functools
import math
import jax
import jax.numpy as jnp
from jax import lax
from jax.experimental import pallas as pl
from jax.experimental.pallas import tpu as pltpu
from jax.sharding import PartitionSpec as P

MESH = pl.DeviceIdType.MESH
F32 = jnp.float32
BF16 = jnp.bfloat16
NQ = 8
CT = 1024
CUT = 1
CH = 512
R = 9


def torus(n):
    side = max(1, math.isqrt(n // 2))
    return n // (2 * side), side


def peer(n, k):
    rows, side = torus(n)
    me = lax.axis_index('sp')
    core = lax.rem(me + k % 2, 2)
    col = lax.rem(lax.rem(lax.div(me, 2), side) + k // 2 % side, side)
    row = lax.rem(lax.div(me, 2 * side) + k // (2 * side), rows)
    return (row * side + col) * 2 + core


def far_first(n, ks):
    rows, side = torus(n)

    def hops(k):
        a, b = k // 2 % side, k // (2 * side)
        return min(a, side - a) + min(b, rows - b)
    return sorted(ks, key=lambda k: (-hops(k), k % 2, k))


def barrier(n):
    sem = pltpu.get_barrier_semaphore()
    for k in far_first(n, range(1, n)):
        pl.semaphore_signal(sem, 1, device_id={'sp': peer(n, k)}, device_id_type=MESH)
    return sem


def all_of(refs, sem):
    pltpu.make_async_copy(refs, refs, sem).wait()


class Softmax:
    def __init__(self, q2, kt, vb, row0, lim, s_ref, hk):
        nh, dh = q2.shape[0] // 2, q2.shape[1] // 2
        self.nh, self.dh, self.kt, self.vb, self.lim, self.s = nh, dh, kt, vb, lim - row0, s_ref
        self.row0 = row0
        self.c2 = dh ** -0.5 * math.log2(math.e)
        self.q2 = q2
        row = lax.broadcasted_iota(jnp.int32, (nh, 128), 0) // hk
        self.lane = lax.broadcasted_iota(jnp.int32, (nh, 128), 1)
        self.lane = jnp.where(row == lax.rem(self.lane, hk), self.lane, 2**30)
        self.mx = jnp.full((nh, 128), -jnp.inf, F32)
        self.l = jnp.zeros((nh, 128), F32)
        self.o = jnp.zeros((2 * nh, 2 * dh), F32)

    def scores(self, i):
        nh, half = self.nh, CH // 2
        r = self.row0 + i
        k2 = jnp.concatenate([self.kt[:, r:r + half], self.kt[:, r + half:r + CH]], axis=0)
        s = jnp.dot(self.q2[...], k2, preferred_element_type=F32)
        for u in range(2):
            for e in range(0, half, 128):
                se = jnp.where(self.lane < self.lim - (i + u * half + e), s[u * nh:(u + 1) * nh, e:e + 128], -jnp.inf)
                self.mx = jnp.maximum(self.mx, se)
                self.s[u * nh:(u + 1) * nh, i // 2 + e:i // 2 + e + 128] = se

    def maximum(self):
        self.m = self.mx.max(1, keepdims=True) * self.c2
        self.safe = jnp.where(self.m == -jnp.inf, 0.0, self.m)

    def values(self, i):
        nh, half = self.nh, CH // 2
        ps = []
        for u in range(2):
            row = []
            for e in range(0, half, 128):
                p = jnp.exp2(self.s[u * nh:(u + 1) * nh, i // 2 + e:i // 2 + e + 128] * self.c2 - self.safe)
                self.l = self.l + p
                row.append(p.astype(BF16))
            ps.append(jnp.concatenate(row, axis=1))
        r = self.row0 + i
        v2 = jnp.concatenate([self.vb[r:r + half], self.vb[r + half:r + CH]], axis=1)
        self.o = self.o + jnp.dot(jnp.concatenate(ps, axis=0), v2, preferred_element_type=F32)

    def result(self):
        nh, dh = self.nh, self.dh
        return self.m, self.l.sum(1, keepdims=True), self.o[:nh, :dh] + self.o[nh:, dh:]


def merge(parts):
    m = functools.reduce(jnp.maximum, [p[0] for p in parts])
    safe = jnp.where(m == -jnp.inf, 0.0, m)
    w = [jnp.exp2(p[0] - safe) for p in parts]
    return m, sum(a * p[1] for a, p in zip(w, parts)), sum(a * p[2] for a, p in zip(w, parts))


def put(n, nb, b, m, l, o, om, ob):
    nh, dh = o.shape
    ob[...] = o
    for h in range(2):
        om[:, h * nb + b, :] = ob[pl.ds(h, n, stride=2), :]
    glane = lax.broadcasted_iota(jnp.int32, (nh, dh), 1)
    at = lax.rem(lax.broadcasted_iota(jnp.int32, (nh, dh), 0), 2) * nb + b
    return jnp.where(glane == at, m, 0.0) + jnp.where(glane == 2 * nb + at, l, 0.0)


def stats_row(n, g, gb):
    gb[...] = g
    return gb[pl.ds(0, n, stride=2), :] + gb[pl.ds(1, n, stride=2), :]


def decode(n, posh, x, wq, wk, wv, wo, kc, vc, yo, rw, kv, vv,
           qall, kvn, xb, wqb, wkvb, qs, kvs, part, theirs, perm_ref, q2, kt, s_ref, ob, gb, om, wob, orx, ys, yrx, yb,
           pos, psem, xsem, wsem, csem, osem, ps, pr, qss, qrs, kss, krs, os_, or_, ys_, yr_, gs_, gr_):
    me = lax.axis_index('sp')
    nb, d = x.shape
    cols = wqb.shape[1]
    half = wkvb.shape[0]
    r = lax.rem(me, 2)
    t = lax.div(me, 2)
    heads = wk.shape[1] // 128
    row0 = pl.multiple_of(r * half, half)
    xcp = pltpu.make_async_copy(x, xb, xsem)
    xcp.start()
    pcp = pltpu.make_async_copy(posh, pos, psem)
    pcp.start()

    @pl.when(t < heads)
    def _():
        pltpu.make_async_copy(wk.at[pl.ds(row0, half), pl.ds(pl.multiple_of(t * 128, 128), 128)], wkvb, wsem.at[NQ]).start()

    @pl.when(t >= heads)
    def _():
        pltpu.make_async_copy(wv.at[pl.ds(row0, half), pl.ds(pl.multiple_of((t - heads) * 128, 128), 128)], wkvb, wsem.at[NQ]).start()
    step = d // NQ
    wcp = [pltpu.make_async_copy(wq.at[pl.ds(i * step, step), pl.ds(pl.multiple_of(me * cols, cols), cols)],
                                 wqb.at[pl.ds(i * step, step)], wsem.at[i]) for i in range(NQ)]
    for c in wcp:
        c.start()
    bar = barrier(n)
    ccp = [pltpu.make_async_copy(f.at[b], t_.at[b], csem.at[e, b]) for e, (f, t_) in enumerate(((kc, kv), (vc, vv)))
           for b in range(nb)]
    xcp.wait()
    pcp.wait()
    pltpu.make_async_copy(wk.at[pl.ds(0, half), pl.ds(0, 128)], wkvb, wsem.at[NQ]).wait()
    kvp = jnp.dot(xb[:, pl.ds(row0, half)], wkvb[...], preferred_element_type=F32)
    part[...] = jnp.concatenate([kvp, kvp], axis=0)
    swap = pltpu.make_async_remote_copy(part, theirs, ps, pr, device_id={'sp': me + 1 - 2 * r}, device_id_type=MESH)
    q = jnp.zeros((nb, cols), F32)
    for i in range(NQ):
        wcp[i].wait()
        if i == NQ - 3:
            for c in ccp[:nb]:
                c.start()
        q = q + jnp.dot(xb[:, i * step:(i + 1) * step], wqb[i * step:(i + 1) * step], preferred_element_type=F32)
    qs[...] = jnp.concatenate([q[:, :128], q[:, 128:]], axis=0).astype(BF16)
    qall[me] = qs[...]
    pl.semaphore_wait(bar, n - 1)
    swap.start()

    for k in far_first(n, range(1, n)):
        pltpu.make_async_remote_copy(qs, qall.at[me], qss, qrs, device_id={'sp': peer(n, k)}, device_id_type=MESH).start()
    swap.wait()
    kvs[...] = (part[...] + theirs[...]).astype(BF16)
    kvn[t] = kvs[...]

    for k in far_first(n, range(2, n, 2)):
        pltpu.make_async_remote_copy(kvs, kvn.at[t], kss, krs, device_id={'sp': peer(n, k)}, device_id_type=MESH).start()
    wcp_o = pltpu.make_async_copy(wo, wob, osem)
    _, rows, dh = kv.shape
    hk = rw.shape[1]
    sl = rows // hk
    nh = 2 * n
    start = me * sl
    m_ = nb * nh
    i0 = lax.broadcasted_iota(jnp.int32, (m_, m_), 0)
    i1 = lax.broadcasted_iota(jnp.int32, (m_, m_), 1)
    want = (lax.rem(i0, nh) // 2) * (2 * nb) + lax.rem(i0, 2) * nb + i0 // nh
    perm_ref[...] = (i1 == want).astype(F32).astype(BF16)
    for b in range(nb):
        ccp[b].wait()
        ccp[nb + b].start()
        for i in range(0, kv.shape[1], CT):
            kt[b, :, i:i + CT] = kv[b, i:i + CT].T
    all_of(qall.at[pl.ds(0, n - 1)], qrs)
    wcp_o.start()
    qb = jnp.dot(perm_ref[...], qall[...].reshape(m_, dh), preferred_element_type=F32).astype(BF16)
    for b in range(nb):
        for u in range(2):
            q2[b, u * nh:(u + 1) * nh, u * dh:(u + 1) * dh] = qb[b * nh:(b + 1) * nh]
            q2[b, u * nh:(u + 1) * nh, (1 - u) * dh:(2 - u) * dh] = jnp.zeros((nh, dh), BF16)
    g = jnp.zeros((nh, dh), F32)
    cut = rows // CUT
    at = [Softmax(q2.at[i // CUT], kt.at[i // CUT], vv.at[i // CUT], i % CUT * cut, (pos[i // CUT] - start) * hk, s_ref.at[i % 2], hk)
          for i in range(nb * CUT)]
    for e in range(nb * CUT + 1):
        if e and (e - 1) % CUT == 0:
            ccp[nb + (e - 1) // CUT].wait()
        for i in range(0, cut, CH):
            if e < nb * CUT:
                at[e].scores(i)
            if e:
                at[e - 1].values(i)
        if e < nb * CUT:
            at[e].maximum()
        if e and e % CUT == 0:
            b = e // CUT - 1
            g = g + put(n, nb, b, *merge([a.result() for a in at[b * CUT:e]]), om, ob)
    om[:, 2 * nb, :] = stats_row(n, g, gb)
    cols = wo.shape[1] // n
    for k in far_first(n, range(1, n)):
        to = peer(n, k)
        pltpu.make_async_remote_copy(om.at[to], orx.at[me], os_, or_,
                                     device_id={'sp': to}, device_id_type=MESH).start()
    orx[me] = om[me]
    all_of(qall.at[pl.ds(0, n - 1)], qss)
    all_of(kvn.at[pl.ds(0, n // 2 - 1)], kss)
    all_of(kvn.at[pl.ds(0, n // 2 - 1)], krs)
    nt = kvn.shape[0]
    j0 = lax.broadcasted_iota(jnp.int32, (nt * nb, nt * 2 * nb), 0)
    j1 = lax.broadcasted_iota(jnp.int32, (nt * nb, nt * 2 * nb), 1)
    want2 = ((j0 // (nb * hk)) * hk + lax.rem(j0, hk)) * 2 * nb + lax.rem(j0 // hk, nb)
    perm2 = (j1 == want2).astype(F32).astype(BF16)
    rw[...] = jnp.dot(perm2, kvn[...].reshape(nt * 2 * nb, dh), preferred_element_type=F32).astype(BF16).reshape(2 * nb, hk, dh)
    kh = lax.div(me * hk, n)
    knew = kvn[kh].astype(F32)
    vnew = kvn[hk + kh].astype(F32)
    snew = (qall[me].astype(F32) * knew).sum(1, keepdims=True) * (dh ** -0.5 * math.log2(math.e))
    all_of(om.at[pl.ds(0, n - 1)], os_)
    all_of(orx.at[pl.ds(0, n - 1)], or_)
    st = orx[:, 2 * nb, :].T
    m = st[0:2 * nb]
    l = st[2 * nb:4 * nb]
    top = jnp.maximum(m.max(1, keepdims=True), snew)
    a = jnp.exp2(m - top)
    anew = jnp.exp2(snew - top)
    den = (a * l).sum(1, keepdims=True) + anew
    num = anew * vnew
    for i in range(n):
        num = num + a[:, i:i + 1] * orx[i, 0:2 * nb, :]
    o = (num / den)
    o = jnp.concatenate([o[:nb], o[nb:]], axis=1).astype(BF16)
    wcp_o.wait()
    order = far_first(n, range(n))
    cut = sorted({0, n // 8, n // 4, n // 2, 3 * n // 4, n})
    groups = [order[i:j] for i, j in zip(cut, cut[1:])] + [[]]
    before = []
    for group in groups:
        for k in group:
            to = peer(n, k)
            w = wob[:, pl.ds(pl.multiple_of(to * cols, cols), cols)]
            part = jnp.dot(o, w, preferred_element_type=F32)
            part = jnp.concatenate([part[:, :128], part[:, 128:]], axis=0)
            if k:
                ys[to] = part
            else:
                yrx[me] = part
        for k in before:
            if k:
                to = peer(n, k)
                pltpu.make_async_remote_copy(ys.at[to], yrx.at[me], ys_, yr_, device_id={'sp': to}, device_id_type=MESH).start()
        before = group
    all_of(ys.at[pl.ds(0, n - 1)], ys_)
    all_of(yrx.at[pl.ds(0, n - 1)], yr_)
    yb[...] = yrx[...].sum(0).astype(BF16)
    yo[me] = yb[...]

    for k in far_first(n, range(1, n)):
        pltpu.make_async_remote_copy(yb, yo.at[me], gs_, gr_, device_id={'sp': peer(n, k)}, device_id_type=MESH).start()
    all_of(yo.at[pl.ds(0, n - 1)], gs_)
    all_of(yo.at[pl.ds(0, n - 1)], gr_)


def store(n, pos, rw, y, kv, vv, ko, vo, yo, k2, v2, sem, ysem):
    nb, rows, _ = kv.shape
    hk = rw.shape[1]
    sl = rows // hk
    start = lax.axis_index('sp') * sl

    def bulk(b):
        return (pltpu.make_async_copy(k2.at[b], ko.at[b], sem.at[0, b]), pltpu.make_async_copy(v2.at[b], vo.at[b], sem.at[1, b]))

    def begin(b, own):
        at = pos[b] - start
        here = (at >= 0) & (at < sl)

        @pl.when(here if own else jnp.logical_not(here))
        def _():
            for i in range(0, rows, rows // 16):
                cut = pl.ds(i, rows // 16)
                pltpu.make_async_copy(k2.at[b, cut], ko.at[b, cut], sem.at[0, b]).start()
                pltpu.make_async_copy(v2.at[b, cut], vo.at[b, cut], sem.at[1, b]).start()
    for b in range(nb):
        at = pos[b] - start

        @pl.when((at >= 0) & (at < sl))
        def _():
            here = pl.ds(pl.multiple_of(at * hk, hk), hk)
            k2[b, here] = rw[b]
            v2[b, here] = rw[nb + b]
    for own in (False, True):
        for b in range(nb):
            begin(b, own)
    ycp = pltpu.make_async_copy(y, yo, ysem)
    ycp.start()
    ycp.wait()
    for b in range(nb):
        for a in bulk(b):
            a.wait()


def solution(mesh):
    n = mesh.shape['sp']
    vm = pl.BlockSpec(memory_space=pltpu.VMEM)
    hbm = pl.BlockSpec(memory_space=pltpu.HBM)
    sm = pl.BlockSpec(memory_space=pltpu.SMEM)
    dma = pltpu.SemaphoreType.DMA

    def params(i, mib):
        return pltpu.CompilerParams(collective_id=i, has_side_effects=i is not None, vmem_limit_bytes=mib * 2**20)

    def local(x, wq, wk, wv, wo, kc, vc, pos, lens):
        nb, d = x.shape
        _, sl, hk, dh = kc.shape
        cols = wq.shape[1] // n
        nt = 2 * hk
        half = d * nt // n
        kc = kc.reshape(nb, sl * hk, dh)
        vc = vc.reshape(nb, sl * hk, dh)
        shape = kc.shape
        x, wq, wk, wv, wo, kc, vc = (pltpu.with_memory_space_constraint(a, pltpu.HBM) for a in (x, wq, wk, wv, wo, kc, vc))
        small = (2 * nb, dh)
        y, rw, kv, vv = pl.pallas_call(
            functools.partial(decode, n),
            out_shape=[pltpu.VMEM((n,) + small, BF16), pltpu.VMEM((2 * nb, hk, dh), BF16), pltpu.VMEM(shape, BF16), pltpu.VMEM(shape, BF16)],
            in_specs=[hbm] * 8, out_specs=[vm] * 4,
            scratch_shapes=[pltpu.VMEM((n,) + small, BF16), pltpu.VMEM((nt,) + small, BF16),
                            pltpu.VMEM((nb, d), BF16), pltpu.VMEM((d, cols), BF16), pltpu.VMEM((half, dh), BF16),
                            pltpu.VMEM(small, BF16), pltpu.VMEM(small, BF16), pltpu.VMEM(small, F32), pltpu.VMEM(small, F32),
                            pltpu.VMEM((n * 2 * nb, n * 2 * nb), BF16), pltpu.VMEM((nb, 4 * n, 2 * dh), BF16), pltpu.VMEM((nb, dh, sl * hk), BF16), pltpu.VMEM((2, 4 * n, sl * hk // 2), F32),
                            pltpu.VMEM((2 * n, dh), F32), pltpu.VMEM((2 * n, dh), F32), pltpu.VMEM((n, R, dh), F32),
                            pltpu.VMEM(wo.shape, BF16), pltpu.VMEM((n, R, dh), F32), pltpu.VMEM((n,) + small, F32),
                            pltpu.VMEM((n,) + small, F32), pltpu.VMEM(small, BF16),
                            pltpu.SMEM((nb,), jnp.int32), dma, dma, dma((NQ + 1,)), dma((2, nb)), dma] + [dma] * 12,
            compiler_params=params(0, 36), name='decode')(pltpu.with_memory_space_constraint(pos, pltpu.HBM), x, wq, wk, wv, wo, kc, vc)
        ko, vo, y, _, _ = pl.pallas_call(
            functools.partial(store, n),
            out_shape=[jax.ShapeDtypeStruct(shape, BF16), jax.ShapeDtypeStruct(shape, BF16), jax.ShapeDtypeStruct(y.shape, BF16),
                       pltpu.VMEM(shape, BF16), pltpu.VMEM(shape, BF16)],
            in_specs=[sm, vm, vm, vm, vm], out_specs=[hbm, hbm, hbm, vm, vm],
            input_output_aliases={3: 3, 4: 4},
            scratch_shapes=[dma((2, nb)), dma],
            compiler_params=params(None, 4), name='store')(pos, rw, y, kv, vv)
        y = y.reshape(n, 2, nb, dh).transpose(2, 0, 1, 3).reshape(nb, -1)
        return y, ko.reshape(nb, sl, hk, dh), vo.reshape(nb, sl, hk, dh)

    cache = P('dp', 'sp', None, None)
    return jax.shard_map(
        local, mesh=mesh,
        in_specs=(P('dp', None), P(None, None), P(None, None), P(None, None), P('sp', None),
                  cache, cache, P('dp'), P('dp')),
        out_specs=(P('dp', None), cache, cache),
        check_vma=False)
```

```python
import functools
import math
import jax
import jax.numpy as jnp
from jax import lax
from jax.experimental import pallas as pl
from jax.experimental.pallas import tpu as pltpu
from jax.sharding import PartitionSpec as P

MESH = pl.DeviceIdType.MESH
F32 = jnp.float32
BF16 = jnp.bfloat16
NQ = 8
CT = 1024
CUT = 1
CH = 512
R = 9


def torus(n):
    side = max(1, math.isqrt(n // 2))
    return n // (2 * side), side


def peer(n, k):
    rows, side = torus(n)
    me = lax.axis_index('sp')
    core = lax.rem(me + k % 2, 2)
    col = lax.rem(lax.rem(lax.div(me, 2), side) + k // 2 % side, side)
    row = lax.rem(lax.div(me, 2 * side) + k // (2 * side), rows)
    return (row * side + col) * 2 + core


def far_first(n, ks):
    rows, side = torus(n)

    def hops(k):
        a, b = k // 2 % side, k // (2 * side)
        return min(a, side - a) + min(b, rows - b)
    return sorted(ks, key=lambda k: (-hops(k), k % 2, k))


def barrier(n):
    sem = pltpu.get_barrier_semaphore()
    for k in far_first(n, range(1, n)):
        pl.semaphore_signal(sem, 1, device_id={'sp': peer(n, k)}, device_id_type=MESH)
    return sem


def all_of(refs, sem):
    pltpu.make_async_copy(refs, refs, sem).wait()


class Softmax:
    def __init__(self, q2, kt, vb, row0, lim, s_ref, hk):
        nh, dh = q2.shape[0] // 2, q2.shape[1] // 2
        self.nh, self.dh, self.kt, self.vb, self.lim, self.s = nh, dh, kt, vb, lim - row0, s_ref
        self.row0 = row0
        self.c2 = dh ** -0.5 * math.log2(math.e)
        self.q2 = q2
        row = lax.broadcasted_iota(jnp.int32, (nh, 128), 0) // hk
        self.lane = lax.broadcasted_iota(jnp.int32, (nh, 128), 1)
        self.lane = jnp.where(row == lax.rem(self.lane, hk), self.lane, 2**30)
        self.mx = jnp.full((nh, 128), -jnp.inf, F32)
        self.l = jnp.zeros((nh, 128), F32)
        self.o = jnp.zeros((2 * nh, 2 * dh), F32)

    def scores(self, i):
        nh, half = self.nh, CH // 2
        r = self.row0 + i
        k2 = jnp.concatenate([self.kt[:, r:r + half], self.kt[:, r + half:r + CH]], axis=0)
        s = jnp.dot(self.q2[...], k2, preferred_element_type=F32)
        for u in range(2):
            for e in range(0, half, 128):
                se = jnp.where(self.lane < self.lim - (i + u * half + e), s[u * nh:(u + 1) * nh, e:e + 128], -jnp.inf)
                self.mx = jnp.maximum(self.mx, se)
                self.s[u * nh:(u + 1) * nh, i // 2 + e:i // 2 + e + 128] = se

    def maximum(self):
        self.m = self.mx.max(1, keepdims=True) * self.c2
        self.safe = jnp.where(self.m == -jnp.inf, 0.0, self.m)

    def values(self, i):
        nh, half = self.nh, CH // 2
        ps = []
        for u in range(2):
            row = []
            for e in range(0, half, 128):
                p = jnp.exp2(self.s[u * nh:(u + 1) * nh, i // 2 + e:i // 2 + e + 128] * self.c2 - self.safe)
                self.l = self.l + p
                row.append(p.astype(BF16))
            ps.append(jnp.concatenate(row, axis=1))
        r = self.row0 + i
        v2 = jnp.concatenate([self.vb[r:r + half], self.vb[r + half:r + CH]], axis=1)
        self.o = self.o + jnp.dot(jnp.concatenate(ps, axis=0), v2, preferred_element_type=F32)

    def result(self):
        nh, dh = self.nh, self.dh
        return self.m, self.l.sum(1, keepdims=True), self.o[:nh, :dh] + self.o[nh:, dh:]


def merge(parts):
    m = functools.reduce(jnp.maximum, [p[0] for p in parts])
    safe = jnp.where(m == -jnp.inf, 0.0, m)
    w = [jnp.exp2(p[0] - safe) for p in parts]
    return m, sum(a * p[1] for a, p in zip(w, parts)), sum(a * p[2] for a, p in zip(w, parts))


def put(n, nb, b, m, l, o, om, ob):
    nh, dh = o.shape
    ob[...] = o
    for h in range(2):
        om[:, h * nb + b, :] = ob[pl.ds(h, n, stride=2), :]
    glane = lax.broadcasted_iota(jnp.int32, (nh, dh), 1)
    at = lax.rem(lax.broadcasted_iota(jnp.int32, (nh, dh), 0), 2) * nb + b
    return jnp.where(glane == at, m, 0.0) + jnp.where(glane == 2 * nb + at, l, 0.0)


def stats_row(n, g, gb):
    gb[...] = g
    return gb[pl.ds(0, n, stride=2), :] + gb[pl.ds(1, n, stride=2), :]


def decode(n, posh, x, wq, wk, wv, wo, kc, vc, yo, rw, kv, vv,
           qall, kvn, xb, wqb, wkvb, qs, kvs, part, theirs, perm_ref, q2, kt, s_ref, ob, gb, om, wob, orx, ys, yrx, yb,
           pos, psem, xsem, wsem, csem, osem, ps, pr, qss, qrs, kss, krs, os_, or_, ys_, yr_, gs_, gr_):
    me = lax.axis_index('sp')
    nb, d = x.shape
    cols = wqb.shape[1]
    half = wkvb.shape[0]
    r = lax.rem(me, 2)
    t = lax.div(me, 2)
    heads = wk.shape[1] // 128
    row0 = pl.multiple_of(r * half, half)
    xcp = pltpu.make_async_copy(x, xb, xsem)
    xcp.start()
    pcp = pltpu.make_async_copy(posh, pos, psem)
    pcp.start()

    @pl.when(t < heads)
    def _():
        pltpu.make_async_copy(wk.at[pl.ds(row0, half), pl.ds(pl.multiple_of(t * 128, 128), 128)], wkvb, wsem.at[NQ]).start()

    @pl.when(t >= heads)
    def _():
        pltpu.make_async_copy(wv.at[pl.ds(row0, half), pl.ds(pl.multiple_of((t - heads) * 128, 128), 128)], wkvb, wsem.at[NQ]).start()
    step = d // NQ
    wcp = [pltpu.make_async_copy(wq.at[pl.ds(i * step, step), pl.ds(pl.multiple_of(me * cols, cols), cols)],
                                 wqb.at[pl.ds(i * step, step)], wsem.at[i]) for i in range(NQ)]
    for c in wcp:
        c.start()
    bar = barrier(n)
    ccp = [pltpu.make_async_copy(f.at[b], t_.at[b], csem.at[e, b]) for e, (f, t_) in enumerate(((kc, kv), (vc, vv)))
           for b in range(nb)]
    xcp.wait()
    pcp.wait()
    pltpu.make_async_copy(wk.at[pl.ds(0, half), pl.ds(0, 128)], wkvb, wsem.at[NQ]).wait()
    kvp = jnp.dot(xb[:, pl.ds(row0, half)], wkvb[...], preferred_element_type=F32)
    part[...] = jnp.concatenate([kvp, kvp], axis=0)
    swap = pltpu.make_async_remote_copy(part, theirs, ps, pr, device_id={'sp': me + 1 - 2 * r}, device_id_type=MESH)
    q = jnp.zeros((nb, cols), F32)
    for i in range(NQ):
        wcp[i].wait()
        if i == NQ - 3:
            for c in ccp[:nb]:
                c.start()
        q = q + jnp.dot(xb[:, i * step:(i + 1) * step], wqb[i * step:(i + 1) * step], preferred_element_type=F32)
    qs[...] = jnp.concatenate([q[:, :128], q[:, 128:]], axis=0).astype(BF16)
    qall[me] = qs[...]
    pl.semaphore_wait(bar, n - 1)
    swap.start()

    for k in far_first(n, range(1, n)):
        pltpu.make_async_remote_copy(qs, qall.at[me], qss, qrs, device_id={'sp': peer(n, k)}, device_id_type=MESH).start()
    swap.wait()
    kvs[...] = (part[...] + theirs[...]).astype(BF16)
    kvn[t] = kvs[...]

    for k in far_first(n, range(2, n, 2)):
        pltpu.make_async_remote_copy(kvs, kvn.at[t], kss, krs, device_id={'sp': peer(n, k)}, device_id_type=MESH).start()
    wcp_o = pltpu.make_async_copy(wo, wob, osem)
    _, rows, dh = kv.shape
    hk = rw.shape[1]
    sl = rows // hk
    nh = 2 * n
    start = me * sl
    m_ = nb * nh
    i0 = lax.broadcasted_iota(jnp.int32, (m_, m_), 0)
    i1 = lax.broadcasted_iota(jnp.int32, (m_, m_), 1)
    want = (lax.rem(i0, nh) // 2) * (2 * nb) + lax.rem(i0, 2) * nb + i0 // nh
    perm_ref[...] = (i1 == want).astype(F32).astype(BF16)
    for b in range(nb):
        ccp[b].wait()
        ccp[nb + b].start()
        for i in range(0, kv.shape[1], CT):
            kt[b, :, i:i + CT] = kv[b, i:i + CT].T
    all_of(qall.at[pl.ds(0, n - 1)], qrs)
    wcp_o.start()
    qb = jnp.dot(perm_ref[...], qall[...].reshape(m_, dh), preferred_element_type=F32).astype(BF16)
    for b in range(nb):
        for u in range(2):
            q2[b, u * nh:(u + 1) * nh, u * dh:(u + 1) * dh] = qb[b * nh:(b + 1) * nh]
            q2[b, u * nh:(u + 1) * nh, (1 - u) * dh:(2 - u) * dh] = jnp.zeros((nh, dh), BF16)
    g = jnp.zeros((nh, dh), F32)
    cut = rows // CUT
    at = [Softmax(q2.at[i // CUT], kt.at[i // CUT], vv.at[i // CUT], i % CUT * cut, (pos[i // CUT] - start) * hk, s_ref.at[i % 2], hk)
          for i in range(nb * CUT)]
    for e in range(nb * CUT + 1):
        if e and (e - 1) % CUT == 0:
            ccp[nb + (e - 1) // CUT].wait()
        for i in range(0, cut, CH):
            if e < nb * CUT:
                at[e].scores(i)
            if e:
                at[e - 1].values(i)
        if e < nb * CUT:
            at[e].maximum()
        if e and e % CUT == 0:
            b = e // CUT - 1
            g = g + put(n, nb, b, *merge([a.result() for a in at[b * CUT:e]]), om, ob)
    om[:, 2 * nb, :] = stats_row(n, g, gb)
    cols = wo.shape[1] // n
    for k in far_first(n, range(1, n)):
        to = peer(n, k)
        pltpu.make_async_remote_copy(om.at[to], orx.at[me], os_, or_,
                                     device_id={'sp': to}, device_id_type=MESH).start()
    orx[me] = om[me]
    all_of(qall.at[pl.ds(0, n - 1)], qss)
    all_of(kvn.at[pl.ds(0, n // 2 - 1)], kss)
    all_of(kvn.at[pl.ds(0, n // 2 - 1)], krs)
    nt = kvn.shape[0]
    j0 = lax.broadcasted_iota(jnp.int32, (nt * nb, nt * 2 * nb), 0)
    j1 = lax.broadcasted_iota(jnp.int32, (nt * nb, nt * 2 * nb), 1)
    want2 = ((j0 // (nb * hk)) * hk + lax.rem(j0, hk)) * 2 * nb + lax.rem(j0 // hk, nb)
    perm2 = (j1 == want2).astype(F32).astype(BF16)
    rw[...] = jnp.dot(perm2, kvn[...].reshape(nt * 2 * nb, dh), preferred_element_type=F32).astype(BF16).reshape(2 * nb, hk, dh)
    kh = lax.div(me * hk, n)
    knew = kvn[kh].astype(F32)
    vnew = kvn[hk + kh].astype(F32)
    snew = (qall[me].astype(F32) * knew).sum(1, keepdims=True) * (dh ** -0.5 * math.log2(math.e))
    all_of(om.at[pl.ds(0, n - 1)], os_)
    all_of(orx.at[pl.ds(0, n - 1)], or_)
    st = orx[:, 2 * nb, :].T
    m = st[0:2 * nb]
    l = st[2 * nb:4 * nb]
    top = jnp.maximum(m.max(1, keepdims=True), snew)
    a = jnp.exp2(m - top)
    anew = jnp.exp2(snew - top)
    den = (a * l).sum(1, keepdims=True) + anew
    num = anew * vnew
    for i in range(n):
        num = num + a[:, i:i + 1] * orx[i, 0:2 * nb, :]
    o = (num / den)
    o = jnp.concatenate([o[:nb], o[nb:]], axis=1).astype(BF16)
    wcp_o.wait()
    order = far_first(n, range(n))
    cut = sorted({0, n // 8, n // 4, n // 2, 3 * n // 4, n})
    groups = [order[i:j] for i, j in zip(cut, cut[1:])] + [[]]
    before = []
    for group in groups:
        for k in group:
            to = peer(n, k)
            w = wob[:, pl.ds(pl.multiple_of(to * cols, cols), cols)]
            part = jnp.dot(o, w, preferred_element_type=F32)
            part = jnp.concatenate([part[:, :128], part[:, 128:]], axis=0)
            if k:
                ys[to] = part
            else:
                yrx[me] = part
        for k in before:
            if k:
                to = peer(n, k)
                pltpu.make_async_remote_copy(ys.at[to], yrx.at[me], ys_, yr_, device_id={'sp': to}, device_id_type=MESH).start()
        before = group
    all_of(ys.at[pl.ds(0, n - 1)], ys_)
    all_of(yrx.at[pl.ds(0, n - 1)], yr_)
    yb[...] = yrx[...].sum(0).astype(BF16)
    yo[me] = yb[...]

    for k in far_first(n, range(1, n)):
        pltpu.make_async_remote_copy(yb, yo.at[me], gs_, gr_, device_id={'sp': peer(n, k)}, device_id_type=MESH).start()
    all_of(yo.at[pl.ds(0, n - 1)], gs_)
    all_of(yo.at[pl.ds(0, n - 1)], gr_)


def store(n, pos, rw, y, kv, vv, ko, vo, yo, k2, v2, sem, ysem):
    nb, rows, _ = kv.shape
    hk = rw.shape[1]
    sl = rows // hk
    start = lax.axis_index('sp') * sl
    pos = [pos[0, b] for b in range(nb)]

    def bulk(b):
        return (pltpu.make_async_copy(k2.at[b], ko.at[b], sem.at[0, b]), pltpu.make_async_copy(v2.at[b], vo.at[b], sem.at[1, b]))

    def begin(b, own):
        at = pos[b] - start
        here = (at >= 0) & (at < sl)

        @pl.when(here if own else jnp.logical_not(here))
        def _():
            for i in range(0, rows, rows // 16):
                cut = pl.ds(i, rows // 16)
                pltpu.make_async_copy(k2.at[b, cut], ko.at[b, cut], sem.at[0, b]).start()
                pltpu.make_async_copy(v2.at[b, cut], vo.at[b, cut], sem.at[1, b]).start()
    for b in range(nb):
        at = pos[b] - start

        @pl.when((at >= 0) & (at < sl))
        def _():
            here = pl.ds(pl.multiple_of(at * hk, hk), hk)
            k2[b, here] = rw[b]
            v2[b, here] = rw[nb + b]
    for own in (False, True):
        for b in range(nb):
            begin(b, own)
    ycp = pltpu.make_async_copy(y, yo, ysem)
    ycp.start()
    ycp.wait()
    for b in range(nb):
        for a in bulk(b):
            a.wait()


def solution(mesh):
    n = mesh.shape['sp']
    vm = pl.BlockSpec(memory_space=pltpu.VMEM)
    hbm = pl.BlockSpec(memory_space=pltpu.HBM)
    sm = pl.BlockSpec(memory_space=pltpu.SMEM)
    dma = pltpu.SemaphoreType.DMA

    def params(i, mib):
        return pltpu.CompilerParams(collective_id=i, has_side_effects=i is not None, vmem_limit_bytes=mib * 2**20)

    def local(x, wq, wk, wv, wo, kc, vc, pos, lens):
        nb, d = x.shape
        _, sl, hk, dh = kc.shape
        cols = wq.shape[1] // n
        nt = 2 * hk
        half = d * nt // n
        kc = kc.reshape(nb, sl * hk, dh)
        vc = vc.reshape(nb, sl * hk, dh)
        shape = kc.shape
        x, wq, wk, wv, wo, kc, vc = (pltpu.with_memory_space_constraint(a, pltpu.HBM) for a in (x, wq, wk, wv, wo, kc, vc))
        small = (2 * nb, dh)
        y, rw, kv, vv = pl.pallas_call(
            functools.partial(decode, n),
            out_shape=[pltpu.VMEM((n,) + small, BF16), pltpu.VMEM((2 * nb, hk, dh), BF16), pltpu.VMEM(shape, BF16), pltpu.VMEM(shape, BF16)],
            in_specs=[hbm] * 8, out_specs=[vm] * 4,
            scratch_shapes=[pltpu.VMEM((n,) + small, BF16), pltpu.VMEM((nt,) + small, BF16),
                            pltpu.VMEM((nb, d), BF16), pltpu.VMEM((d, cols), BF16), pltpu.VMEM((half, dh), BF16),
                            pltpu.VMEM(small, BF16), pltpu.VMEM(small, BF16), pltpu.VMEM(small, F32), pltpu.VMEM(small, F32),
                            pltpu.VMEM((n * 2 * nb, n * 2 * nb), BF16), pltpu.VMEM((nb, 4 * n, 2 * dh), BF16), pltpu.VMEM((nb, dh, sl * hk), BF16), pltpu.VMEM((2, 4 * n, sl * hk // 2), F32),
                            pltpu.VMEM((2 * n, dh), F32), pltpu.VMEM((2 * n, dh), F32), pltpu.VMEM((n, R, dh), F32),
                            pltpu.VMEM(wo.shape, BF16), pltpu.VMEM((n, R, dh), F32), pltpu.VMEM((n,) + small, F32),
                            pltpu.VMEM((n,) + small, F32), pltpu.VMEM(small, BF16),
                            pltpu.SMEM((nb,), jnp.int32), dma, dma, dma((NQ + 1,)), dma((2, nb)), dma] + [dma] * 12,
            compiler_params=params(0, 36), name='decode')(pltpu.with_memory_space_constraint(pos, pltpu.HBM), x, wq, wk, wv, wo, kc, vc)
        ko, vo, y, _, _ = pl.pallas_call(
            functools.partial(store, n),
            out_shape=[jax.ShapeDtypeStruct(shape, BF16), jax.ShapeDtypeStruct(shape, BF16), jax.ShapeDtypeStruct(y.shape, BF16),
                       pltpu.VMEM(shape, BF16), pltpu.VMEM(shape, BF16)],
            in_specs=[vm, vm, vm, vm, vm], out_specs=[hbm, hbm, hbm, vm, vm],
            input_output_aliases={3: 3, 4: 4},
            scratch_shapes=[dma((2, nb)), dma],
            compiler_params=params(None, 4), name='store')(pos.reshape(1, nb), rw, y, kv, vv)
        y = y.reshape(n, 2, nb, dh).transpose(2, 0, 1, 3).reshape(nb, -1)
        return y, ko.reshape(nb, sl, hk, dh), vo.reshape(nb, sl, hk, dh)

    cache = P('dp', 'sp', None, None)
    return jax.shard_map(
        local, mesh=mesh,
        in_specs=(P('dp', None), P(None, None), P(None, None), P(None, None), P('sp', None),
                  cache, cache, P('dp'), P('dp')),
        out_specs=(P('dp', None), cache, cache),
        check_vma=False)
```
